128 devices in a mesh: band: 8 (over y, x_lo), chan: 16 (over x_hi, z, core).
Axes of the slice: x: 4 (x_hi: 2, x_lo: 2; x = x_hi * 2 + x_lo), y: 4, z: 4, core: 2. Of those that a mesh axis runs over, the one named last changes fastest.
Arguments:
- coeffs: bfloat16 [2, 8, 1024, 8192], P(None, None, 'chan', 'band'), may hold values from -1100 to 1100, as said below
Outputs:
- coherence: float32 [1024, 1024], P('chan', 'band')
The draws below stay inside these ranges and needn't reach their ends.
Inputs may be any that keep to these rules, and one draw needn't show every extreme that they name: `coeffs`: finite real and imaginary parts.
All inputs are finite; a program needn't handle non-finite values.
Results may differ from the reference program's by a relative error of at most 0.0003.
Values may be sent and summed in bfloat16 or wider, within the bound.
A program may use at most 192 MiB of HBM per device.

```python
import jax
import jax.numpy as jnp
from jax import lax

C = 1024
K = 8
W = 16
BINS = 8192


def draw_coeffs(key, part):
    noise_key = jax.random.fold_in(jax.random.fold_in(key, 17), 0)
    noise = jnp.clip(jax.random.normal(noise_key, (2, K, C, BINS), jnp.float32), -6.0, 6.0)
    values = noise
    return values.astype(jnp.bfloat16)


def setup_inputs(seed: int = 0) -> dict:
    splits = jax.random.split(jax.random.key(seed), 2)
    return {
        "coeffs": draw_coeffs(jax.random.fold_in(splits[1], 71), 0),
    }


epsilon = 1e-6


def band_term(total, block):
    width = block.shape[2]
    flat = block.transpose(2, 0, 1, 3).reshape(width, -1)
    paired = jnp.stack((block[1], -block[0]), axis=0).transpose(2, 0, 1, 3).reshape(width, -1)
    real_part = jnp.dot(flat, flat.T, preferred_element_type=jnp.float32)
    imag_part = jnp.dot(paired, flat.T, preferred_element_type=jnp.float32)
    wide = flat.astype(jnp.float32)
    power = jnp.sum(wide * wide, axis=1) + epsilon
    coh_band = (real_part * real_part + imag_part * imag_part) / (power[:, None] * power[None, :])
    return total + coh_band, None


def reference(coeffs):
    num_bands = BINS // W
    width = coeffs.shape[2]
    blocks = coeffs.reshape(2, K, width, num_bands, W)
    blocks = jnp.moveaxis(blocks, 3, 0)
    total, unused = lax.scan(band_term, jnp.zeros((width, width), jnp.float32), blocks)
    rows = lax.broadcasted_iota(jnp.int32, (width, width), 0)
    cols = lax.broadcasted_iota(jnp.int32, (width, width), 1)
    total = jnp.where(rows == cols, jnp.float32(0.0), total)
    return total * jnp.float32(W * K / num_bands)
```

```python
import functools

import jax
import jax.numpy as jnp
from jax import lax
from jax.experimental import pallas as pl
from jax.experimental.pallas import tpu as pltpu
from jax.sharding import PartitionSpec as P

K = 8
W = 16
EPS = 1e-06
MESH = pl.DeviceIdType.MESH
TILES = 36
F32 = jnp.float32
BF16 = jnp.bfloat16


def nt_dot(a, b):
    return lax.dot_general(a, b, (((1,), (1,)), ((), ())), preferred_element_type=F32)


def relayout(src, dst):
    group = lax.broadcasted_iota(jnp.int32, (16, 128), 1) // 16
    bits = [(group // (1 << s)) % 2 == 1 for s in range(3)]
    for part in range(2):
        for r in range(4):
            rows = pl.ds(r * 16, 16)
            vals = []
            for k in range(8):
                v = src[part, k, rows, :].astype(F32)
                vals.append(v if k == 0 else pltpu.roll(v, 16 * k, 1))
            for s in range(3):
                vals = [jnp.where(bits[s], vals[(m + (1 << s)) % 8], vals[m]) for m in range(8)]
            for w in range(8):
                dst[w, rows, part * 128 : (part + 1) * 128] = vals[(8 - w) % 8].astype(BF16)


def split_square(x):
    wide = x.astype(F32)
    square = wide * wide
    high = square.astype(BF16)
    low = (square - high.astype(F32)).astype(BF16)
    return high, low


def kernel(
    scale, cx, out, xin, sbuf, rbuf, lhs, rowi, coli, tacc, yrecv, fsend, frecv, bpad, bt, drecv,
    in_s, p1s, p1r, fws, fwr, ys, yr, fs, fr, ds, dr,
):
    b = lax.axis_index("band")
    ch = lax.axis_index("chan")
    y, xlo = b // 2, b % 2
    g, c = ch // 2, ch % 2
    xhi, z = g // 4, g % 4
    x = xhi * 2 + xlo
    pc = 1 - c

    def member(k):
        return lax.rem(xhi + k // 4, 2) * 4 + lax.rem(z + k, 4)

    def target(k):
        return lax.rem(xhi + k // 4, 2) * 4 + lax.rem(z + 8 - k, 4)

    def dev(band, grp, core):
        return (band, grp * 2 + core)

    barrier = pltpu.get_barrier_semaphore()
    for k in range(1, 8):
        pl.semaphore_signal(barrier, inc=1, device_id=dev(b, target(k), c), device_id_type=MESH)
    pl.semaphore_signal(barrier, inc=1, device_id=dev(b, g, pc), device_id_type=MESH)
    for r in range(1, 4):
        pl.semaphore_signal(
            barrier, inc=1, device_id=dev(lax.rem(y + r, 4) * 2 + xlo, g, c), device_id_type=MESH
        )
    for d in (1, 3):
        xo = lax.rem(x + d, 4)
        pl.semaphore_signal(
            barrier,
            inc=1,
            device_id=dev(y * 2 + xo % 2, (xo // 2) * 4 + z, c),
            device_id_type=MESH,
        )

    def load(k):
        return pltpu.make_async_copy(
            cx.at[:, :, :, pl.ds(pl.multiple_of(target(k) * 128, 128), 128)], xin.at[k], in_s.at[k]
        )

    for k in range(1, 8):
        load(k).start()
    load(0).start()

    def p1(k):
        return pltpu.make_async_remote_copy(
            src_ref=sbuf.at[k],
            dst_ref=rbuf.at[k, c],
            send_sem=p1s.at[k],
            recv_sem=p1r.at[k],
            device_id=dev(b, target(k), c),
            device_id_type=MESH,
        )

    def fwd(k):
        return pltpu.make_async_remote_copy(
            src_ref=rbuf.at[k, c],
            dst_ref=rbuf.at[k, c],
            send_sem=fws.at[k],
            recv_sem=fwr.at[k],
            device_id=dev(b, g, pc),
            device_id_type=MESH,
        )

    def send_loop(k, carry):
        load(k).wait()
        relayout(xin.at[k], sbuf.at[k])

        @pl.when(k == 1)
        def _():
            pl.semaphore_wait(barrier, 13)

        p1(k).start()
        return carry

    lax.fori_loop(1, 8, send_loop, 0)
    load(0).wait()
    relayout(xin.at[0], rbuf.at[0, c])
    fwd(0).start()

    ones_row = jnp.ones((8, 256), BF16)
    ones_col = jnp.ones((128, 256), BF16)

    def ysend(t):
        yt = lax.rem(t, 4)
        return pltpu.make_async_remote_copy(
            src_ref=tacc.at[t],
            dst_ref=yrecv.at[t // 4, lax.rem(y + 3 - yt + 4, 4)],
            send_sem=ys.at[t],
            recv_sem=yr.at[t // 4, lax.rem(y + 3 - yt + 4, 4)],
            device_id=dev(yt * 2 + xlo, g, c),
            device_id_type=MESH,
        )

    def tile(i, j):
        t = i * (i + 1) // 2 + j
        acc = jnp.zeros((64, 128), F32)
        for w in range(8):
            right = rbuf[j, :, w].reshape(128, 256)
            prod = nt_dot(lhs[w], right)
            re, im = prod[:64], prod[64:]
            acc = acc + (re * re + im * im) * (coli[w] * rowi[j, w, 0:1, :])
        tacc[t] = acc

        @pl.when(lax.rem(t, 4) != y)
        def _():
            ysend(t).start()

    def step(i, carry):
        @pl.when(i > 0)
        def _():
            p1(i).wait_recv()
            fwd(i).start()

        for w in range(8):
            v = rbuf[i, c, w]
            lhs[w, 0:64, :] = v
            lhs[w, 64:128, 0:128] = v[:, 128:]
            lhs[w, 64:128, 128:256] = -v[:, :128]
            high, low = split_square(v)
            coli[w] = 1.0 / (nt_dot(high, ones_col) + nt_dot(low, ones_col) + EPS)

        def inner(j, carry2):
            tile(i, j)
            return carry2

        lax.fori_loop(0, i, inner, 0)
        fwd(i).wait_recv()
        for w in range(8):
            high, low = split_square(rbuf[i, :, w].reshape(128, 256))
            rowi[i, w] = 1.0 / (nt_dot(ones_row, high) + nt_dot(ones_row, low) + EPS)
        tile(i, i)
        return carry

    lax.fori_loop(0, 8, step, 0)

    slot = x * 4 + z

    def pair_of(t):
        i = 0
        for m in range(1, 8):
            i = i + jnp.where(t >= m * (m + 1) // 2, 1, 0)
        return i, t - i * (i + 1) // 2

    def fsend_copy(q, side, band, grp):
        return pltpu.make_async_remote_copy(
            src_ref=fsend.at[q],
            dst_ref=frecv.at[slot],
            send_sem=fs.at[q, side],
            recv_sem=fr.at[slot],
            device_id=dev(band, grp, c),
            device_id_type=MESH,
        )

    def is_self(band, grp):
        return jnp.where(band == b, 1, 0) * jnp.where(grp == g, 1, 0)

    def final_loop(q, carry):
        t = q * 4 + y
        i, j = pair_of(t)
        s, u = member(i), member(j)
        total = tacc[t]
        for r in range(3):
            pltpu.make_async_remote_copy(
                src_ref=tacc.at[t],
                dst_ref=yrecv.at[q, r],
                send_sem=ys.at[t],
                recv_sem=yr.at[q, r],
                device_id=dev(b, g, c),
                device_id_type=MESH,
            ).wait_recv()
            total = total + yrecv[q, r]
        fsend[q] = total

        @pl.when(is_self(u, s) == 1)
        def _():
            frecv[slot] = total

        @pl.when(is_self(u, s) == 0)
        def _():
            fsend_copy(q, 0, u, s).start()

        @pl.when((i != j) & (is_self(s, u) == 1))
        def _():
            frecv[slot] = total

        @pl.when((i != j) & (is_self(s, u) == 0))
        def _():
            fsend_copy(q, 1, s, u).start()

        return carry

    lax.fori_loop(0, 9, final_loop, 0)

    def collect(s, carry):
        straight_sum, mirror_sum = carry
        xs, zs = s // 4, lax.rem(s, 4)
        xh = xs // 2
        kr = lax.rem(xhi + 2 - xh, 2) * 4 + lax.rem(z + 4 - zs, 4)
        kc = lax.rem(b // 4 + 2 - xh, 2) * 4 + lax.rem(lax.rem(b, 4) + 4 - zs, 4)
        hi, lo = jnp.maximum(kr, kc), jnp.minimum(kr, kc)
        yt = lax.rem(hi * (hi + 1) // 2 + lo, 4)
        mine = jnp.where(s == slot, 1, 0) * jnp.where(yt == y, 1, 0)

        @pl.when(mine == 0)
        def _():
            pltpu.make_async_remote_copy(
                src_ref=fsend.at[0],
                dst_ref=frecv.at[s],
                send_sem=fs.at[0, 0],
                recv_sem=fr.at[s],
                device_id=dev(b, g, c),
                device_id_type=MESH,
            ).wait_recv()

        value = frecv[s]
        straight = jnp.where(kr >= kc, 1, 0).astype(F32)
        return straight_sum + value * straight, mirror_sum + value * (1.0 - straight)

    zero = jnp.zeros((64, 128), F32)
    straight_sum, mirror_sum = lax.fori_loop(0, 16, collect, (zero, zero))
    bpad[...] = jnp.zeros((128, 128), F32)
    bpad[pl.ds(pl.multiple_of(c * 64, 64), 64), :] = mirror_sum
    bt[...] = bpad[...].T
    swap = pltpu.make_async_remote_copy(
        src_ref=bt.at[pl.ds(pl.multiple_of(pc * 64, 64), 64)],
        dst_ref=drecv,
        send_sem=ds,
        recv_sem=dr,
        device_id=dev(b, g, pc),
        device_id_type=MESH,
    )
    swap.start()
    value = straight_sum + bt[pl.ds(pl.multiple_of(c * 64, 64), 64), :]
    swap.wait_recv()
    value = (value + drecv[...]) * scale
    row = lax.broadcasted_iota(jnp.int32, (64, 128), 0) + (g * 128 + c * 64)
    col = lax.broadcasted_iota(jnp.int32, (64, 128), 1) + b * 128
    out[...] = jnp.where(row == col, jnp.float32(0.0), value)

    swap.wait_send()
    for k in range(1, 8):
        p1(k).wait_send()
    for k in range(8):
        fwd(k).wait_send()

    def drain_y(t, carry):
        @pl.when(lax.rem(t, 4) != y)
        def _():
            ysend(t).wait_send()

        return carry

    lax.fori_loop(0, TILES, drain_y, 0)

    def drain_f(q, carry):
        i, j = pair_of(q * 4 + y)
        s, u = member(i), member(j)

        @pl.when(is_self(u, s) == 0)
        def _():
            fsend_copy(q, 0, u, s).wait_send()

        @pl.when((i != j) & (is_self(s, u) == 0))
        def _():
            fsend_copy(q, 1, s, u).wait_send()

        return carry

    lax.fori_loop(0, 9, drain_f, 0)


def body(coeffs):
    num_bands = coeffs.shape[3] // W * lax.axis_size("band")
    scale = W * K / num_bands
    dma = pltpu.SemaphoreType.DMA
    return pl.pallas_call(
        functools.partial(kernel, scale),
        name="coherence",
        out_shape=jax.ShapeDtypeStruct((64, 128), F32),
        in_specs=[pl.BlockSpec(memory_space=pl.ANY)],
        out_specs=pl.BlockSpec(memory_space=pltpu.VMEM),
        scratch_shapes=[
            pltpu.VMEM((8, 2, 8, 64, 128), BF16),
            pltpu.VMEM((8, 8, 64, 256), BF16),
            pltpu.VMEM((8, 2, 8, 64, 256), BF16),
            pltpu.VMEM((8, 128, 256), BF16),
            pltpu.VMEM((8, 8, 8, 128), F32),
            pltpu.VMEM((8, 64, 128), F32),
            pltpu.VMEM((TILES, 64, 128), F32),
            pltpu.VMEM((9, 3, 64, 128), F32),
            pltpu.VMEM((9, 64, 128), F32),
            pltpu.VMEM((16, 64, 128), F32),
            pltpu.VMEM((128, 128), F32),
            pltpu.VMEM((128, 128), F32),
            pltpu.VMEM((64, 128), F32),
            dma((8,)),
            dma((8,)),
            dma((8,)),
            dma((8,)),
            dma((8,)),
            dma((TILES,)),
            dma((9, 3)),
            dma((9, 2)),
            dma((16,)),
            dma,
            dma,
        ],
        compiler_params=pltpu.CompilerParams(
            collective_id=0, has_side_effects=True, vmem_limit_bytes=48 * 2**20
        ),
    )(coeffs)


def solution(mesh):
    return jax.shard_map(
        body,
        mesh=mesh,
        in_specs=(P(None, None, "chan", "band"),),
        out_specs=P("chan", "band"),
        check_vma=False,
    )
```

```python
import functools

import jax
import jax.numpy as jnp
from jax import lax
from jax.experimental import pallas as pl
from jax.experimental.pallas import tpu as pltpu
from jax.sharding import PartitionSpec as P

K = 8
W = 16
EPS = 1e-06
MESH = pl.DeviceIdType.MESH
TILES = 36
F32 = jnp.float32
BF16 = jnp.bfloat16


def nt_dot(a, b):
    return lax.dot_general(a, b, (((1,), (1,)), ((), ())), preferred_element_type=F32)


def relayout(src, dst):
    group = lax.broadcasted_iota(jnp.int32, (16, 128), 1) // 16
    bits = [(group // (1 << s)) % 2 == 1 for s in range(3)]
    for part in range(2):
        for r in range(4):
            rows = pl.ds(r * 16, 16)
            vals = []
            for k in range(8):
                v = src[part, k, rows, :].astype(F32)
                vals.append(v if k == 0 else pltpu.roll(v, 16 * k, 1))
            for s in range(3):
                vals = [jnp.where(bits[s], vals[(m + (1 << s)) % 8], vals[m]) for m in range(8)]
            for w in range(8):
                dst[w, rows, part * 128 : (part + 1) * 128] = vals[(8 - w) % 8].astype(BF16)


def split_square(x):
    wide = x.astype(F32)
    square = wide * wide
    high = square.astype(BF16)
    low = (square - high.astype(F32)).astype(BF16)
    return high, low


RANK = (0, 4, 2, 7, 1, 6, 3, 5)
ISSUE = (4, 3, 2, 7, 6, 1, 5)
GROUPS = ((0, 4), (1, 7), (2, 6), (3, 5))
PHASES = ((0, 1, 2, 3, 4), (5,), (6,), (7,))


def lookup(table, index):
    value = 0
    for n, entry in enumerate(table):
        if entry:
            value = value + jnp.where(index == n, entry, 0)
    return value


def spans(first, last):
    out, j = [], first
    for size in (4, 2, 1):
        while j + size <= last:
            out.append((j, size))
            j += size
    return out


def slot_of(i, j):
    return i * (i + 1) // 2 + j


def group_tiles(group, steps):
    return [(i, j) for i in steps for j in GROUPS[group] if j <= i]


def kernel(
    scale, cx, out, xin, sbuf, rbuf, lhs, squares, prow, precv, rowi, coli, xt, tacc, yrecv, fsend, frecv,
    bpad, bt, drecv, in_s, p1s, p1r, fws, fwr, pps, ppr, ys, yr, fs, fr, ds, dr,
):
    b = lax.axis_index("band")
    ch = lax.axis_index("chan")
    y, xlo = b // 2, b % 2
    g, c = ch // 2, ch % 2
    xhi, z = g // 4, g % 4
    x = xhi * 2 + xlo
    pc = 1 - c

    flipped = (z, z + 1 - 2 * lax.rem(z, 2), lax.rem(z + 2, 4), 3 - z)

    def member(k):
        return lax.rem(xhi + k // 4, 2) * 4 + flipped[k % 4]

    def dev(band, grp, core):
        return (band, grp * 2 + core)

    barrier = pltpu.get_barrier_semaphore()
    for dx in range(4):
        for dz in range(4):
            if dx or dz:
                xo, zo = lax.rem(x + dx, 4), lax.rem(z + dz, 4)
                pl.semaphore_signal(
                    barrier,
                    inc=1,
                    device_id=dev(y * 2 + xo % 2, (xo // 2) * 4 + zo, c),
                    device_id_type=MESH,
                )
    pl.semaphore_signal(barrier, inc=1, device_id=dev(b, g, pc), device_id_type=MESH)
    for r in range(1, 4):
        pl.semaphore_signal(
            barrier, inc=1, device_id=dev(lax.rem(y + r, 4) * 2 + xlo, g, c), device_id_type=MESH
        )

    order = ISSUE + (0,)
    load_parts = ((0, 1), (1, 2), (3, 5))

    def load(n, part):
        at = pl.multiple_of(member(order[n]) * 128, 128)
        return pltpu.make_async_copy(cx.at[:, :, :, pl.ds(at, 128)], xin.at[n], in_s.at[part])

    for part, (first, count) in enumerate(load_parts):
        for n in range(first, first + count):
            load(n, part).start()

    def load_wait(part):
        first, count = load_parts[part]
        block = xin.at[pl.ds(first, count)]
        pltpu.make_async_copy(block, block, in_s.at[part]).wait()

    def p1(k):
        rank = RANK.index(k)
        return pltpu.make_async_remote_copy(
            src_ref=sbuf.at[k],
            dst_ref=rbuf.at[rank, c],
            send_sem=p1s,
            recv_sem=p1r.at[rank],
            device_id=dev(b, member(k), c),
            device_id_type=MESH,
        )

    def fwd(i):
        return pltpu.make_async_remote_copy(
            src_ref=rbuf.at[i, c],
            dst_ref=rbuf.at[i, c],
            send_sem=fws,
            recv_sem=fwr.at[i],
            device_id=dev(b, g, pc),
            device_id_type=MESH,
        )

    def pfwd(i):
        return pltpu.make_async_remote_copy(
            src_ref=prow.at[i],
            dst_ref=precv.at[i],
            send_sem=pps,
            recv_sem=ppr.at[i],
            device_id=dev(b, g, pc),
            device_id_type=MESH,
        )

    with jax.named_scope("relayout"):
        load_wait(0)
        relayout(xin.at[0], sbuf.at[ISSUE[0]])
        load_wait(1)
        for n in (1, 2):
            relayout(xin.at[n], sbuf.at[ISSUE[n]])
    with jax.named_scope("bar"):
        pl.semaphore_wait(barrier, 19)
    for k in ISSUE[:3]:
        p1(k).start()
    with jax.named_scope("relayout2"):
        load_wait(2)
        for n in range(3, 7):
            relayout(xin.at[n], sbuf.at[ISSUE[n]])
            p1(ISSUE[n]).start()
    relayout(xin.at[7], rbuf.at[0, c])
    fwd(0).start()

    ones_col = jnp.ones((128, 256), BF16)
    band_row = lax.broadcasted_iota(jnp.int32, (8, 128), 0)
    own_lane = (
        lax.broadcasted_iota(jnp.int32, (64, 128), 0) + c * 64
        == lax.broadcasted_iota(jnp.int32, (64, 128), 1)
    )

    chunks = [member(k) for k in RANK]

    planes = [chunks[group[0]] // 2 for group in GROUPS]
    group_of = {j: n for n, group in enumerate(GROUPS) for j in group}
    phase_of = {i: n for n, steps in enumerate(PHASES) for i in steps}
    slot = x * 4 + z

    def bulk(count, send_sem, recv_sem):
        block = tacc.at[pl.ds(0, count)]
        return pltpu.make_async_remote_copy(
            src_ref=block,
            dst_ref=block,
            send_sem=send_sem,
            recv_sem=recv_sem,
            device_id=dev(b, g, pc),
            device_id_type=MESH,
        )

    def ysend(i, j):
        group = group_of[j]
        at = lax.rem(y + 7 - planes[group], 4)
        return pltpu.make_async_remote_copy(
            src_ref=tacc.at[slot_of(i, j)],
            dst_ref=yrecv.at[slot_of(i, j), at],
            send_sem=ys.at[i // 7, group],
            recv_sem=yr.at[phase_of[i], at],
            device_id=dev(planes[group] * 2 + xlo, g, c),
            device_id_type=MESH,
        )

    def ysent(late, steps):
        for group in range(4):

            @pl.when(y != planes[group])
            def _():
                bulk(len(group_tiles(group, steps)), ys.at[late, group], fr).wait_send()

    def tiles(i, first, count):
        width = 128 * min(count, 2)
        for j in range(first, first + count, 2):
            acc = jnp.zeros((64, width), F32)
            for w in range(8):
                if j == 7:
                    prod = nt_dot(lhs[w], rbuf[j, :, w].reshape(width, 256))
                else:
                    prod = jnp.dot(
                        lhs[w],
                        xt[w, :, j * 128 : j * 128 + width],
                        preferred_element_type=F32,
                    )
                re, im = prod[:64], prod[64:]
                col = coli[w]
                if width == 256:
                    col = jnp.concatenate((col, col), axis=1)
                acc = acc + (re * re + im * im) * (
                    col * rowi[w : w + 1, j * 128 : j * 128 + width]
                )
            for n in range(width // 128):
                tacc[slot_of(i, j + n)] = acc[:, n * 128 : (n + 1) * 128]
        for j in range(first, first + count):

            @pl.when(y != planes[group_of[j]])
            def _():
                ysend(i, j).start()

    def fsend_copy(i, j, side):
        row, col = (chunks[i], chunks[j]) if side == 0 else (chunks[j], chunks[i])
        return pltpu.make_async_remote_copy(
            src_ref=fsend.at[slot_of(i, j)],
            dst_ref=frecv.at[slot],
            send_sem=fs,
            recv_sem=fr,
            device_id=dev(col, row, c),
            device_id_type=MESH,
        )

    def is_own(i, j):
        return (b == chunks[j]) & (g == chunks[i])

    def mirror(i, j):
        if i == j:
            return
        if j != 0:
            fsend_copy(i, j, 1).start()
            return

        @pl.when(jnp.logical_not(is_own(j, i)))
        def _():
            fsend_copy(i, j, 1).start()

    def final(phase, mirrored):
        for group in range(4):

            @pl.when(y == planes[group])
            def _():
                members = group_tiles(group, PHASES[phase])
                with jax.named_scope(f"wait_y{phase}"):
                    for r in range(3):
                        bulk(len(members), fs, yr.at[phase, r]).wait_recv()
                for i, j in members:
                    t = slot_of(i, j)
                    total = tacc[t]
                    for r in range(3):
                        total = total + yrecv[t, r]
                    fsend[t] = total
                    if j != 0:
                        fsend_copy(i, j, 0).start()
                    elif i != 0:
                        fsend_copy(i, j, 0).start()

                        @pl.when(is_own(j, i))
                        def _():
                            frecv[slot] = total
                    else:

                        @pl.when(is_own(i, j))
                        def _():
                            frecv[slot] = total

                        @pl.when(jnp.logical_not(is_own(i, j)))
                        def _():
                            fsend_copy(i, j, 0).start()

                    if mirrored:
                        mirror(i, j)

    for i in range(8):
        if i > 0:
            with jax.named_scope(f"wait_p1_{i}"):
                p1(RANK[i]).wait_recv()
            fwd(i).start()
        if i == 7:
            with jax.named_scope("final_a"):
                final(0, False)
        with jax.named_scope("power"):
            for w in range(8):
                v = rbuf[i, c, w]
                lhs[w, 0:64, :] = v
                lhs[w, 64:128, 0:128] = v[:, 128:]
                lhs[w, 64:128, 128:256] = -v[:, :128]
                squares[0, w], squares[1, w] = split_square(v)
            sums = nt_dot(squares[...].reshape(1024, 256), ones_col)
            sums = sums[:512] + sums[512:] + EPS
            coli[...] = (1.0 / sums).reshape(8, 64, 128)
            row = jnp.zeros((8, 128), F32)
            for w in range(8):
                own = jnp.where(own_lane, sums[w * 64 : (w + 1) * 64], 0.0)
                own = jnp.sum(own, axis=0, keepdims=True)
                row = jnp.where(band_row == w, own, row)
            prow[i] = row
            pfwd(i).start()
        before = i if i == 7 else i // 2 * 2
        with jax.named_scope("tiles"):
            for first, count in spans(0, before):
                tiles(i, first, count)
        with jax.named_scope("wait_fwd"):
            fwd(i).wait_recv()
            pfwd(i).wait_recv()
        with jax.named_scope("tiles_last"):
            rowi[:, i * 128 : (i + 1) * 128] = 1.0 / (prow[i] + precv[i])
            if i < 7:
                for w in range(8):
                    both = rbuf[i, :, w].reshape(128, 256)
                    xt[w, :, i * 128 : (i + 1) * 128] = both.T
            tiles(i, before, i + 1 - before)

    with jax.named_scope("final_b"):
        final(1, False)
        final(2, False)
    with jax.named_scope("sent_y7"):
        ysent(1, (7,))
    with jax.named_scope("mirror"):
        for group in range(4):

            @pl.when(y == planes[group])
            def _():
                for i, j in group_tiles(group, range(7)):
                    mirror(i, j)

    with jax.named_scope("final_c"):
        final(3, True)

    flags = []
    for s in range(16):
        xs, zs = s // 4, s % 4
        xh = xs // 2
        differ = tuple(zs ^ n for n in range(4))
        kr = lax.rem(g // 4 + xh, 2) * 4 + lookup(differ, lax.rem(g, 4))
        kc = lax.rem(b // 4 + xh, 2) * 4 + lookup(differ, lax.rem(b, 4))
        ranks = tuple(RANK.index(n) for n in range(8))
        kr, kc = lookup(ranks, kr), lookup(ranks, kc)
        flags.append(jnp.where(kr >= kc, 1, 0).astype(F32))

    with jax.named_scope("drain"):
        block = sbuf.at[pl.ds(1, 7)]
        pltpu.make_async_remote_copy(
            src_ref=block,
            dst_ref=block,
            send_sem=p1s,
            recv_sem=p1r.at[0],
            device_id=dev(b, g, pc),
            device_id_type=MESH,
        ).wait_send()
        pltpu.make_async_remote_copy(
            src_ref=sbuf,
            dst_ref=sbuf,
            send_sem=fws,
            recv_sem=p1r.at[0],
            device_id=dev(b, g, pc),
            device_id_type=MESH,
        ).wait_send()
        pltpu.make_async_remote_copy(
            src_ref=prow,
            dst_ref=precv,
            send_sem=pps,
            recv_sem=p1r.at[0],
            device_id=dev(b, g, pc),
            device_id_type=MESH,
        ).wait_send()
        ysent(0, range(7))

    with jax.named_scope("collect"):

        @pl.when(y == planes[0])
        def _():
            bulk(15, fs, fr).wait_recv()

        @pl.when(y != planes[0])
        def _():
            bulk(16, fs, fr).wait_recv()

    straight_sum = jnp.zeros((64, 128), F32)
    mirror_sum = jnp.zeros((64, 128), F32)
    for s, weight in enumerate(flags):
        value = frecv[s]
        straight_sum = straight_sum + value * weight
        mirror_sum = mirror_sum + value * (1.0 - weight)

    bpad[...] = jnp.zeros((128, 128), F32)
    bpad[pl.ds(pl.multiple_of(c * 64, 64), 64), :] = mirror_sum
    bt[...] = bpad[...].T
    swap = pltpu.make_async_remote_copy(
        src_ref=bt.at[pl.ds(pl.multiple_of(pc * 64, 64), 64)],
        dst_ref=drecv,
        send_sem=ds,
        recv_sem=dr,
        device_id=dev(b, g, pc),
        device_id_type=MESH,
    )
    swap.start()
    value = straight_sum + bt[pl.ds(pl.multiple_of(c * 64, 64), 64), :]
    with jax.named_scope("drain_f"):
        for group in range(4):

            @pl.when(y == planes[group])
            def _():
                count = 2 * len(group_tiles(group, range(8))) - 2 - (1 if group == 0 else 0)
                bulk(count, fs, fr).wait_send()

    with jax.named_scope("swap"):
        swap.wait_recv()
    value = (value + drecv[...]) * scale
    row = lax.broadcasted_iota(jnp.int32, (64, 128), 0) + (g * 128 + c * 64)
    col = lax.broadcasted_iota(jnp.int32, (64, 128), 1) + b * 128
    out[...] = jnp.where(row == col, jnp.float32(0.0), value)
    swap.wait_send()


def body(coeffs):
    num_bands = coeffs.shape[3] // W * lax.axis_size("band")
    scale = W * K / num_bands
    dma = pltpu.SemaphoreType.DMA
    return pl.pallas_call(
        functools.partial(kernel, scale),
        name="coherence",
        out_shape=pltpu.VMEM((64, 128), F32),
        in_specs=[pl.BlockSpec(memory_space=pl.ANY)],
        out_specs=pl.BlockSpec(memory_space=pltpu.VMEM),
        scratch_shapes=[
            pltpu.VMEM((8, 2, 8, 64, 128), BF16),
            pltpu.VMEM((8, 8, 64, 256), BF16),
            pltpu.VMEM((8, 2, 8, 64, 256), BF16),
            pltpu.VMEM((8, 128, 256), BF16),
            pltpu.VMEM((2, 8, 64, 256), BF16),
            pltpu.VMEM((8, 8, 128), F32),
            pltpu.VMEM((8, 8, 128), F32),
            pltpu.VMEM((8, 1024), F32),
            pltpu.VMEM((8, 64, 128), F32),
            pltpu.VMEM((8, 256, 1024), BF16),
            pltpu.VMEM((TILES, 64, 128), F32),
            pltpu.VMEM((TILES, 3, 64, 128), F32),
            pltpu.VMEM((TILES, 64, 128), F32),
            pltpu.VMEM((16, 64, 128), F32),
            pltpu.VMEM((128, 128), F32),
            pltpu.VMEM((128, 128), F32),
            pltpu.VMEM((64, 128), F32),
            dma((3,)),
            dma,
            dma((8,)),
            dma,
            dma((8,)),
            dma,
            dma((8,)),
            dma((2, 4)),
            dma((4, 3)),
            dma,
            dma,
            dma,
            dma,
        ],
        compiler_params=pltpu.CompilerParams(
            collective_id=0, has_side_effects=True, vmem_limit_bytes=63 * 2**20
        ),
    )(coeffs)


def solution(mesh):
    return jax.shard_map(
        body,
        mesh=mesh,
        in_specs=(P(None, None, "chan", "band"),),
        out_specs=P("chan", "band"),
        check_vma=False,
    )
```

```python
import functools

import jax
import jax.numpy as jnp
from jax import lax
from jax.experimental import pallas as pl
from jax.experimental.pallas import tpu as pltpu
from jax.sharding import PartitionSpec as P

K = 8
W = 16
EPS = 1e-06
MESH = pl.DeviceIdType.MESH
TILES = 36
F32 = jnp.float32
BF16 = jnp.bfloat16


def nt_dot(a, b):
    return lax.dot_general(a, b, (((1,), (1,)), ((), ())), preferred_element_type=F32)


def relayout(src, dst):
    group = lax.broadcasted_iota(jnp.int32, (16, 128), 1) // 16
    bits = [(group // (1 << s)) % 2 == 1 for s in range(3)]
    for part in range(2):
        for r in range(4):
            rows = pl.ds(r * 16, 16)
            vals = []
            for k in range(8):
                v = src[part, k, rows, :].astype(F32)
                vals.append(v if k == 0 else pltpu.roll(v, 16 * k, 1))
            for s in range(3):
                vals = [jnp.where(bits[s], vals[(m + (1 << s)) % 8], vals[m]) for m in range(8)]
            for w in range(8):
                dst[w, rows, part * 128 : (part + 1) * 128] = vals[(8 - w) % 8].astype(BF16)


RANK = (0, 4, 2, 6, 1, 7, 3, 5)
ISSUE = (4, 2, 3, 6, 7, 1, 5)
GROUPS = ((0, 4), (1, 7), (2, 6), (3, 5))


def lookup(table, index):
    value = 0
    for n, entry in enumerate(table):
        if entry:
            value = value + jnp.where(index == n, entry, 0)
    return value


def spans(first, last):
    out, j = [], first
    for size in (4, 2, 1):
        while j + size <= last:
            out.append((j, size))
            j += size
    return out


def slot_of(i, j):
    return i * (i + 1) // 2 + j


def kernel(
    scale, cx, out, xin, sbuf, rbuf, lhs, prow, precv, rowi, coli, xt, tacc, yrecv, fsend, frecv,
    bpad, bt, whole, drecv, in_s, p1s, p1r, fws, fwr, pps, ppr, ys, yr, fs, fr, ds, dr,
):
    b = lax.axis_index("band")
    ch = lax.axis_index("chan")
    y, xlo = b // 2, b % 2
    g, c = ch // 2, ch % 2
    xhi, z = g // 4, g % 4
    x = xhi * 2 + xlo
    pc = 1 - c

    flipped = (z, z + 1 - 2 * lax.rem(z, 2), lax.rem(z + 2, 4), 3 - z)

    def member(k):
        return lax.rem(xhi + k // 4, 2) * 4 + flipped[k % 4]

    def dev(band, grp, core):
        return (band, grp * 2 + core)

    barrier = pltpu.get_barrier_semaphore()
    for dx in range(4):
        for dz in range(4):
            if dx or dz:
                xo, zo = lax.rem(x + dx, 4), lax.rem(z + dz, 4)
                pl.semaphore_signal(
                    barrier,
                    inc=1,
                    device_id=dev(y * 2 + xo % 2, (xo // 2) * 4 + zo, c),
                    device_id_type=MESH,
                )
    pl.semaphore_signal(barrier, inc=1, device_id=dev(b, g, pc), device_id_type=MESH)
    for r in range(1, 4):
        pl.semaphore_signal(
            barrier, inc=1, device_id=dev(lax.rem(y + r, 4) * 2 + xlo, g, c), device_id_type=MESH
        )

    order = ISSUE + (0,)
    load_parts = ((0, 1), (1, 2), (3, 5))

    def load(n, part):
        at = pl.multiple_of(member(order[n]) * 128, 128)
        return pltpu.make_async_copy(cx.at[:, :, :, pl.ds(at, 128)], xin.at[n], in_s.at[part])

    for part, (first, count) in enumerate(load_parts):
        for n in range(first, first + count):
            load(n, part).start()

    def load_wait(part):
        first, count = load_parts[part]
        block = xin.at[pl.ds(first, count)]
        pltpu.make_async_copy(block, block, in_s.at[part]).wait()

    def p1(k):
        rank = RANK.index(k)
        return pltpu.make_async_remote_copy(
            src_ref=sbuf.at[k],
            dst_ref=rbuf.at[rank, c],
            send_sem=p1s,
            recv_sem=p1r.at[rank],
            device_id=dev(b, member(k), c),
            device_id_type=MESH,
        )

    def fwd(i):
        return pltpu.make_async_remote_copy(
            src_ref=rbuf.at[i, c],
            dst_ref=rbuf.at[i, c],
            send_sem=fws,
            recv_sem=fwr.at[i],
            device_id=dev(b, g, pc),
            device_id_type=MESH,
        )

    def pfwd(i):
        return pltpu.make_async_remote_copy(
            src_ref=prow.at[i],
            dst_ref=precv.at[i],
            send_sem=pps,
            recv_sem=ppr.at[i],
            device_id=dev(b, g, pc),
            device_id_type=MESH,
        )

    with jax.named_scope("relayout"):
        load_wait(0)
        relayout(xin.at[0], sbuf.at[ISSUE[0]])
        load_wait(1)
        for n in (1, 2):
            relayout(xin.at[n], sbuf.at[ISSUE[n]])
    with jax.named_scope("bar"):
        pl.semaphore_wait(barrier, 19)
    for k in ISSUE[:3]:
        p1(k).start()
    with jax.named_scope("relayout2"):
        load_wait(2)
        for n in range(3, 7):
            relayout(xin.at[n], sbuf.at[ISSUE[n]])
            p1(ISSUE[n]).start()
    relayout(xin.at[7], rbuf.at[0, c])
    fwd(0).start()

    band_row = lax.broadcasted_iota(jnp.int32, (8, 128), 0)
    own_lane = (
        lax.broadcasted_iota(jnp.int32, (64, 128), 0) + c * 64
        == lax.broadcasted_iota(jnp.int32, (64, 128), 1)
    )

    chunks = [member(k) for k in RANK]

    group_of = {j: n for n, group in enumerate(GROUPS) for j in group}
    heights = [value // 2 for value in chunks]

    def plane(i, group):
        return lax.rem(heights[i] + heights[GROUPS[group][0]], 4)

    slot = x * 4 + z

    def bulk(count, send_sem, recv_sem):
        block = tacc.at[pl.ds(0, count)]
        return pltpu.make_async_remote_copy(
            src_ref=block,
            dst_ref=block,
            send_sem=send_sem,
            recv_sem=recv_sem,
            device_id=dev(b, g, pc),
            device_id_type=MESH,
        )

    def ysend(i, j):
        at_y = plane(i, group_of[j])
        at = lax.rem(y + 7 - at_y, 4)
        return pltpu.make_async_remote_copy(
            src_ref=tacc.at[slot_of(i, j)],
            dst_ref=yrecv.at[slot_of(i, j), at],
            send_sem=ys.at[i // 7],
            recv_sem=yr.at[i, at],
            device_id=dev(at_y * 2 + xlo, g, c),
            device_id_type=MESH,
        )

    def tiles(i, first, count):
        width = 128 * min(count, 2)
        for j in range(first, first + count, 2):
            acc = jnp.zeros((64, width), F32)
            for w in range(8):
                if j == 7:
                    prod = nt_dot(lhs[w], rbuf[j, :, w].reshape(width, 256))
                else:
                    prod = jnp.dot(
                        lhs[w],
                        xt[w, :, j * 128 : j * 128 + width],
                        preferred_element_type=F32,
                    )
                re, im = prod[:64], prod[64:]
                col = coli[w]
                if width == 256:
                    col = jnp.concatenate((col, col), axis=1)
                acc = acc + (re * re + im * im) * (
                    col * rowi[w : w + 1, j * 128 : j * 128 + width]
                )
            for n in range(width // 128):
                tacc[slot_of(i, j + n)] = acc[:, n * 128 : (n + 1) * 128]
        for j in range(first, first + count):

            @pl.when(y != plane(i, group_of[j]))
            def _():
                ysend(i, j).start()

    def fsend_copy(i, j, side):
        row, col = (chunks[i], chunks[j]) if side == 0 else (chunks[j], chunks[i])
        return pltpu.make_async_remote_copy(
            src_ref=fsend.at[slot_of(i, j)],
            dst_ref=frecv.at[slot],
            send_sem=fs,
            recv_sem=fr,
            device_id=dev(y * 2 + col % 2, row, c),
            device_id_type=MESH,
        )

    def send_owner(i, j, side, total):
        row, col = (i, j) if side == 0 else (j, i)
        if row:
            fsend_copy(i, j, side).start()
            return

        @pl.when(chunks[col] % 2 == xlo)
        def _():
            frecv[slot] = total

        @pl.when(chunks[col] % 2 != xlo)
        def _():
            fsend_copy(i, j, side).start()

    def final(i):
        for group in range(4):
            members = [(i, j) for j in GROUPS[group] if j <= i]
            if members:

                @pl.when(y == plane(i, group))
                def _():
                    with jax.named_scope(f"wait_y{i}"):
                        for r in range(3):
                            bulk(len(members), fs, yr.at[i, r]).wait_recv()
                    for i_, j in members:
                        t = slot_of(i, j)
                        total = tacc[t]
                        for r in range(3):
                            total = total + yrecv[t, r]
                        fsend[t] = total
                        send_owner(i, j, 0, total)
                        if i != j:
                            send_owner(i, j, 1, total)

    for i in range(8):
        if i > 0:
            with jax.named_scope(f"wait_p1_{i}"):
                p1(RANK[i]).wait_recv()
            fwd(i).start()
        with jax.named_scope("power"):
            sums = []
            for w in range(8):
                v = rbuf[i, c, w]
                lhs[w, 0:64, :] = v
                lhs[w, 64:128, 0:128] = v[:, 128:]
                lhs[w, 64:128, 128:256] = -v[:, :128]
                wide = v.astype(F32)
                wide = wide * wide
                total = jnp.sum(wide[:, :128] + wide[:, 128:], axis=1, keepdims=True) + EPS
                sums.append(jnp.broadcast_to(total, (64, 128)))
                coli[w] = jnp.broadcast_to(1.0 / total, (64, 128))
            row = jnp.zeros((8, 128), F32)
            for w in range(8):
                own = jnp.where(own_lane, sums[w], 0.0)
                own = jnp.sum(own, axis=0, keepdims=True)
                row = jnp.where(band_row == w, own, row)
            prow[i] = row
            pfwd(i).start()
        before = i if i == 7 else i // 2 * 2
        with jax.named_scope("tiles"):
            for first, count in spans(0, before):
                tiles(i, first, count)
        if i == 7:
            with jax.named_scope("final_a"):
                for m in range(6):
                    final(m)
        with jax.named_scope("wait_fwd"):
            fwd(i).wait_recv()
            pfwd(i).wait_recv()
        with jax.named_scope("tiles_last"):
            rowi[:, i * 128 : (i + 1) * 128] = 1.0 / (prow[i] + precv[i])
            if i < 7:
                for w in range(8):
                    both = rbuf[i, :, w].reshape(128, 256)
                    xt[w, :, i * 128 : (i + 1) * 128] = both.T
            tiles(i, before, i + 1 - before)

    with jax.named_scope("final_b"):
        final(6)
    with jax.named_scope("final_c"):
        final(7)

    col_chunk = lax.rem(y + 4 - g // 2, 4) * 2 + xlo
    flags = []
    for s in range(16):
        xs, zs = s // 4, s % 4
        xh = xs // 2
        differ = tuple(zs ^ n for n in range(4))
        kr = lax.rem(g // 4 + xh, 2) * 4 + lookup(differ, lax.rem(g, 4))
        kc = lax.rem(col_chunk // 4 + xh, 2) * 4 + lookup(differ, lax.rem(col_chunk, 4))
        ranks = tuple(RANK.index(n) for n in range(8))
        kr, kc = lookup(ranks, kr), lookup(ranks, kc)
        flags.append(jnp.where(kr >= kc, 1, 0).astype(F32))

    with jax.named_scope("drain"):
        block = sbuf.at[pl.ds(1, 7)]
        pltpu.make_async_remote_copy(
            src_ref=block,
            dst_ref=block,
            send_sem=p1s,
            recv_sem=p1r.at[0],
            device_id=dev(b, g, pc),
            device_id_type=MESH,
        ).wait_send()
        pltpu.make_async_remote_copy(
            src_ref=sbuf,
            dst_ref=sbuf,
            send_sem=fws,
            recv_sem=p1r.at[0],
            device_id=dev(b, g, pc),
            device_id_type=MESH,
        ).wait_send()
        pltpu.make_async_remote_copy(
            src_ref=prow,
            dst_ref=precv,
            send_sem=pps,
            recv_sem=p1r.at[0],
            device_id=dev(b, g, pc),
            device_id_type=MESH,
        ).wait_send()
        bulk(6, ys.at[1], fr).wait_send()

        @pl.when(lax.rem(y, 2) == 0)
        def _():
            bulk(20, ys.at[0], fr).wait_send()

        @pl.when(lax.rem(y, 2) == 1)
        def _():
            bulk(22, ys.at[0], fr).wait_send()

    with jax.named_scope("collect"):
        bulk(15, fs, fr).wait_recv()

    straight_sum = jnp.zeros((64, 128), F32)
    mirror_sum = jnp.zeros((64, 128), F32)
    for s, weight in enumerate(flags):
        value = frecv[s]
        straight_sum = straight_sum + value * weight
        mirror_sum = mirror_sum + value * (1.0 - weight)

    bpad[...] = jnp.zeros((128, 128), F32)
    bpad[pl.ds(pl.multiple_of(c * 64, 64), 64), :] = mirror_sum
    bt[...] = bpad[...].T
    whole[...] = straight_sum + bt[pl.ds(pl.multiple_of(c * 64, 64), 64), :]

    def deliver(part):
        src = whole if part == 0 else bt.at[pl.ds(pl.multiple_of(pc * 64, 64), 64)]
        return pltpu.make_async_remote_copy(
            src_ref=src,
            dst_ref=drecv.at[part],
            send_sem=ds,
            recv_sem=dr,
            device_id=dev(col_chunk, g, c if part == 0 else pc),
            device_id_type=MESH,
        )

    deliver(1).start()

    @pl.when(col_chunk == b)
    def _():
        drecv[0] = whole[...]

    @pl.when(col_chunk != b)
    def _():
        deliver(0).start()

    with jax.named_scope("drain_f"):
        bulk(15, fs, fr).wait_send()

    with jax.named_scope("swap"):

        @pl.when(col_chunk == b)
        def _():
            bulk(1, ds, dr).wait()

        @pl.when(col_chunk != b)
        def _():
            bulk(2, ds, dr).wait()

    value = (drecv[0] + drecv[1]) * scale
    row = lax.broadcasted_iota(jnp.int32, (64, 128), 0) + (g * 128 + c * 64)
    col = lax.broadcasted_iota(jnp.int32, (64, 128), 1) + b * 128
    out[...] = jnp.where(row == col, jnp.float32(0.0), value)


def body(coeffs):
    num_bands = coeffs.shape[3] // W * lax.axis_size("band")
    scale = W * K / num_bands
    dma = pltpu.SemaphoreType.DMA
    return pl.pallas_call(
        functools.partial(kernel, scale),
        name="coherence",
        out_shape=pltpu.VMEM((64, 128), F32),
        in_specs=[pl.BlockSpec(memory_space=pl.ANY)],
        out_specs=pl.BlockSpec(memory_space=pltpu.VMEM),
        scratch_shapes=[
            pltpu.VMEM((8, 2, 8, 64, 128), BF16),
            pltpu.VMEM((8, 8, 64, 256), BF16),
            pltpu.VMEM((8, 2, 8, 64, 256), BF16),
            pltpu.VMEM((8, 128, 256), BF16),
            pltpu.VMEM((8, 8, 128), F32),
            pltpu.VMEM((8, 8, 128), F32),
            pltpu.VMEM((8, 1024), F32),
            pltpu.VMEM((8, 64, 128), F32),
            pltpu.VMEM((8, 256, 1024), BF16),
            pltpu.VMEM((TILES, 64, 128), F32),
            pltpu.VMEM((TILES, 3, 64, 128), F32),
            pltpu.VMEM((TILES, 64, 128), F32),
            pltpu.VMEM((16, 64, 128), F32),
            pltpu.VMEM((128, 128), F32),
            pltpu.VMEM((128, 128), F32),
            pltpu.VMEM((64, 128), F32),
            pltpu.VMEM((2, 64, 128), F32),
            dma((3,)),
            dma,
            dma((8,)),
            dma,
            dma((8,)),
            dma,
            dma((8,)),
            dma((2,)),
            dma((8, 3)),
            dma,
            dma,
            dma,
            dma,
        ],
        compiler_params=pltpu.CompilerParams(
            collective_id=0, has_side_effects=True, vmem_limit_bytes=63 * 2**20
        ),
    )(coeffs)


def solution(mesh):
    return jax.shard_map(
        body,
        mesh=mesh,
        in_specs=(P(None, None, "chan", "band"),),
        out_specs=P("chan", "band"),
        check_vma=False,
    )
```

```python
import functools

import jax
import jax.numpy as jnp
from jax import lax
from jax.experimental import pallas as pl
from jax.experimental.pallas import tpu as pltpu
from jax.sharding import PartitionSpec as P

K = 8
W = 16
EPS = 1e-06
MESH = pl.DeviceIdType.MESH
TILES = 36
F32 = jnp.float32
BF16 = jnp.bfloat16


def nt_dot(a, b):
    return lax.dot_general(a, b, (((1,), (1,)), ((), ())), preferred_element_type=F32)


def relayout(src, dst):
    group = lax.broadcasted_iota(jnp.int32, (16, 128), 1) // 16
    bits = [(group // (1 << s)) % 2 == 1 for s in range(3)]
    for part in range(2):
        for r in range(4):
            rows = pl.ds(r * 16, 16)
            vals = []
            for k in range(8):
                v = src[part, k, rows, :].astype(F32)
                vals.append(v if k == 0 else pltpu.roll(v, 16 * k, 1))
            for s in range(3):
                vals = [jnp.where(bits[s], vals[(m + (1 << s)) % 8], vals[m]) for m in range(8)]
            for w in range(8):
                dst[w, rows, part * 128 : (part + 1) * 128] = vals[(8 - w) % 8].astype(BF16)


RANK = (0, 4, 2, 6, 1, 7, 3, 5)
ISSUE = (4, 2, 3, 6, 7, 1, 5)
GROUPS = ((0, 4), (1, 7), (2, 6), (3, 5))


def lookup(table, index):
    value = 0
    for n, entry in enumerate(table):
        if entry:
            value = value + jnp.where(index == n, entry, 0)
    return value


def spans(first, last):
    out, j = [], first
    for size in (4, 2, 1):
        while j + size <= last:
            out.append((j, size))
            j += size
    return out


def slot_of(i, j):
    return i * (i + 1) // 2 + j


def kernel(
    scale, cx, out, xin, sbuf, rbuf, lhs, prow, precv, rowi, coli, xt, tacc, yrecv, fsend, frecv,
    bpad, bt, whole, drecv, in_s, p1s, p1r, fws, fwr, pps, ppr, ys, yr, fs, fr, ds, dr,
):
    b = lax.axis_index("band")
    ch = lax.axis_index("chan")
    y, xlo = b // 2, b % 2
    g, c = ch // 2, ch % 2
    xhi, z = g // 4, g % 4
    x = xhi * 2 + xlo
    pc = 1 - c

    flipped = (z, z + 1 - 2 * lax.rem(z, 2), lax.rem(z + 2, 4), 3 - z)

    def member(k):
        return lax.rem(xhi + k // 4, 2) * 4 + flipped[k % 4]

    def dev(band, grp, core):
        return (band, grp * 2 + core)

    barrier = pltpu.get_barrier_semaphore()
    for dx in range(4):
        for dz in range(4):
            if dx or dz:
                xo, zo = lax.rem(x + dx, 4), lax.rem(z + dz, 4)
                pl.semaphore_signal(
                    barrier,
                    inc=1,
                    device_id=dev(y * 2 + xo % 2, (xo // 2) * 4 + zo, c),
                    device_id_type=MESH,
                )
    pl.semaphore_signal(barrier, inc=1, device_id=dev(b, g, pc), device_id_type=MESH)
    for r in range(1, 4):
        pl.semaphore_signal(
            barrier, inc=1, device_id=dev(lax.rem(y + r, 4) * 2 + xlo, g, c), device_id_type=MESH
        )

    order = ISSUE + (0,)
    load_parts = ((0, 1), (1, 2), (3, 5))

    def load(n, part):
        at = pl.multiple_of(member(order[n]) * 128, 128)
        return pltpu.make_async_copy(cx.at[:, :, :, pl.ds(at, 128)], xin.at[n], in_s.at[part])

    for part, (first, count) in enumerate(load_parts):
        for n in range(first, first + count):
            load(n, part).start()

    def load_wait(part):
        first, count = load_parts[part]
        block = xin.at[pl.ds(first, count)]
        pltpu.make_async_copy(block, block, in_s.at[part]).wait()

    def p1(k):
        rank = RANK.index(k)
        return pltpu.make_async_remote_copy(
            src_ref=sbuf.at[k],
            dst_ref=rbuf.at[rank, c],
            send_sem=p1s,
            recv_sem=p1r.at[rank],
            device_id=dev(b, member(k), c),
            device_id_type=MESH,
        )

    def fwd(i):
        return pltpu.make_async_remote_copy(
            src_ref=rbuf.at[i, c],
            dst_ref=rbuf.at[i, c],
            send_sem=fws,
            recv_sem=fwr.at[i],
            device_id=dev(b, g, pc),
            device_id_type=MESH,
        )

    def pfwd(i):
        return pltpu.make_async_remote_copy(
            src_ref=prow.at[i],
            dst_ref=precv.at[i],
            send_sem=pps,
            recv_sem=ppr.at[i],
            device_id=dev(b, g, pc),
            device_id_type=MESH,
        )

    with jax.named_scope("relayout"):
        load_wait(0)
        relayout(xin.at[0], sbuf.at[ISSUE[0]])
        load_wait(1)
        for n in (1, 2):
            relayout(xin.at[n], sbuf.at[ISSUE[n]])
        load_wait(2)
        for n in range(3, 7):
            relayout(xin.at[n], sbuf.at[ISSUE[n]])
    with jax.named_scope("bar"):
        pl.semaphore_wait(barrier, 19)
    for k in ISSUE:
        p1(k).start()
    relayout(xin.at[7], rbuf.at[0, c])
    fwd(0).start()

    band_row = lax.broadcasted_iota(jnp.int32, (8, 128), 0)
    own_lane = (
        lax.broadcasted_iota(jnp.int32, (64, 128), 0) + c * 64
        == lax.broadcasted_iota(jnp.int32, (64, 128), 1)
    )

    chunks = [member(k) for k in RANK]

    group_of = {j: n for n, group in enumerate(GROUPS) for j in group}
    heights = [value // 2 for value in chunks]

    def plane(i, group):
        return lax.rem(heights[i] + heights[GROUPS[group][0]], 4)

    slot = x * 4 + z

    def bulk(count, send_sem, recv_sem):
        block = tacc.at[pl.ds(0, count)]
        return pltpu.make_async_remote_copy(
            src_ref=block,
            dst_ref=block,
            send_sem=send_sem,
            recv_sem=recv_sem,
            device_id=dev(b, g, pc),
            device_id_type=MESH,
        )

    def ysend(i, j):
        at_y = plane(i, group_of[j])
        at = lax.rem(y + 7 - at_y, 4)
        return pltpu.make_async_remote_copy(
            src_ref=tacc.at[slot_of(i, j)],
            dst_ref=yrecv.at[slot_of(i, j), at],
            send_sem=ys.at[i // 7],
            recv_sem=yr.at[i, at],
            device_id=dev(at_y * 2 + xlo, g, c),
            device_id_type=MESH,
        )

    def tiles(i, first, count):
        width = 128 * min(count, 2)
        for j in range(first, first + count, 2):
            acc = jnp.zeros((64, width), F32)
            for w in range(8):
                if j == 7:
                    prod = nt_dot(lhs[w], rbuf[j, :, w].reshape(width, 256))
                else:
                    prod = jnp.dot(
                        lhs[w],
                        xt[w, :, j * 128 : j * 128 + width],
                        preferred_element_type=F32,
                    )
                re, im = prod[:64], prod[64:]
                col = coli[w]
                if width == 256:
                    col = jnp.concatenate((col, col), axis=1)
                acc = acc + (re * re + im * im) * (
                    col * rowi[w : w + 1, j * 128 : j * 128 + width]
                )
            for n in range(width // 128):
                tacc[slot_of(i, j + n)] = acc[:, n * 128 : (n + 1) * 128]
        for j in range(first, first + count):

            @pl.when(y != plane(i, group_of[j]))
            def _():
                ysend(i, j).start()

    def fsend_copy(i, j, side):
        row, col = (chunks[i], chunks[j]) if side == 0 else (chunks[j], chunks[i])
        return pltpu.make_async_remote_copy(
            src_ref=fsend.at[slot_of(i, j)],
            dst_ref=frecv.at[slot],
            send_sem=fs,
            recv_sem=fr,
            device_id=dev(y * 2 + col % 2, row, c),
            device_id_type=MESH,
        )

    def send_owner(i, j, side, total):
        row, col = (i, j) if side == 0 else (j, i)
        if row:
            fsend_copy(i, j, side).start()
            return

        @pl.when(chunks[col] % 2 == xlo)
        def _():
            frecv[slot] = total

        @pl.when(chunks[col] % 2 != xlo)
        def _():
            fsend_copy(i, j, side).start()

    def final(i):
        for group in range(4):
            members = [(i, j) for j in GROUPS[group] if j <= i]
            if members:

                @pl.when(y == plane(i, group))
                def _():
                    with jax.named_scope(f"wait_y{i}"):
                        for r in range(3):
                            bulk(len(members), fs, yr.at[i, r]).wait_recv()
                    for i_, j in members:
                        t = slot_of(i, j)
                        total = tacc[t]
                        for r in range(3):
                            total = total + yrecv[t, r]
                        fsend[t] = total
                        send_owner(i, j, 0, total)
                        if i != j:
                            send_owner(i, j, 1, total)

    for i in range(8):
        if i > 0:
            with jax.named_scope(f"wait_p1_{i}"):
                p1(RANK[i]).wait_recv()
            fwd(i).start()
        with jax.named_scope("power"):
            sums = []
            for w in range(8):
                v = rbuf[i, c, w]
                lhs[w, 0:64, :] = v
                lhs[w, 64:128, 0:128] = v[:, 128:]
                lhs[w, 64:128, 128:256] = -v[:, :128]
                wide = v.astype(F32)
                wide = wide * wide
                total = jnp.sum(wide[:, :128] + wide[:, 128:], axis=1, keepdims=True) + EPS
                sums.append(jnp.broadcast_to(total, (64, 128)))
                coli[w] = jnp.broadcast_to(1.0 / total, (64, 128))
            row = jnp.zeros((8, 128), F32)
            for w in range(8):
                own = jnp.where(own_lane, sums[w], 0.0)
                own = jnp.sum(own, axis=0, keepdims=True)
                row = jnp.where(band_row == w, own, row)
            prow[i] = row
            pfwd(i).start()
        before = i if i == 7 else i // 2 * 2
        with jax.named_scope("tiles"):
            for first, count in spans(0, before):
                tiles(i, first, count)
        if i == 7:
            with jax.named_scope("final_a"):
                for m in range(5):
                    final(m)
        with jax.named_scope("wait_fwd"):
            fwd(i).wait_recv()
            pfwd(i).wait_recv()
        with jax.named_scope("tiles_last"):
            rowi[:, i * 128 : (i + 1) * 128] = 1.0 / (prow[i] + precv[i])
            if i < 7:
                for w in range(8):
                    both = rbuf[i, :, w].reshape(128, 256)
                    xt[w, :, i * 128 : (i + 1) * 128] = both.T
            tiles(i, before, i + 1 - before)

    with jax.named_scope("final_b"):
        final(5)
        final(6)
    with jax.named_scope("final_c"):
        final(7)

    col_chunk = lax.rem(y + 4 - g // 2, 4) * 2 + xlo
    flags = []
    for s in range(16):
        xs, zs = s // 4, s % 4
        xh = xs // 2
        differ = tuple(zs ^ n for n in range(4))
        kr = lax.rem(g // 4 + xh, 2) * 4 + lookup(differ, lax.rem(g, 4))
        kc = lax.rem(col_chunk // 4 + xh, 2) * 4 + lookup(differ, lax.rem(col_chunk, 4))
        ranks = tuple(RANK.index(n) for n in range(8))
        kr, kc = lookup(ranks, kr), lookup(ranks, kc)
        flags.append(jnp.where(kr >= kc, 1, 0).astype(F32))

    with jax.named_scope("drain"):
        block = sbuf.at[pl.ds(1, 7)]
        pltpu.make_async_remote_copy(
            src_ref=block,
            dst_ref=block,
            send_sem=p1s,
            recv_sem=p1r.at[0],
            device_id=dev(b, g, pc),
            device_id_type=MESH,
        ).wait_send()
        pltpu.make_async_remote_copy(
            src_ref=sbuf,
            dst_ref=sbuf,
            send_sem=fws,
            recv_sem=p1r.at[0],
            device_id=dev(b, g, pc),
            device_id_type=MESH,
        ).wait_send()
        pltpu.make_async_remote_copy(
            src_ref=prow,
            dst_ref=precv,
            send_sem=pps,
            recv_sem=p1r.at[0],
            device_id=dev(b, g, pc),
            device_id_type=MESH,
        ).wait_send()
        bulk(6, ys.at[1], fr).wait_send()

        @pl.when(lax.rem(y, 2) == 0)
        def _():
            bulk(20, ys.at[0], fr).wait_send()

        @pl.when(lax.rem(y, 2) == 1)
        def _():
            bulk(22, ys.at[0], fr).wait_send()

    with jax.named_scope("collect"):
        bulk(15, fs, fr).wait_recv()

    straight_sum = jnp.zeros((64, 128), F32)
    mirror_sum = jnp.zeros((64, 128), F32)
    for s, weight in enumerate(flags):
        value = frecv[s]
        straight_sum = straight_sum + value * weight
        mirror_sum = mirror_sum + value * (1.0 - weight)

    bpad[...] = jnp.zeros((128, 128), F32)
    bpad[pl.ds(pl.multiple_of(c * 64, 64), 64), :] = mirror_sum
    bt[...] = bpad[...].T
    whole[...] = straight_sum + bt[pl.ds(pl.multiple_of(c * 64, 64), 64), :]

    def deliver(part):
        src = whole if part == 0 else bt.at[pl.ds(pl.multiple_of(pc * 64, 64), 64)]
        return pltpu.make_async_remote_copy(
            src_ref=src,
            dst_ref=drecv.at[part],
            send_sem=ds,
            recv_sem=dr,
            device_id=dev(col_chunk, g, c if part == 0 else pc),
            device_id_type=MESH,
        )

    deliver(1).start()

    @pl.when(col_chunk == b)
    def _():
        drecv[0] = whole[...]

    @pl.when(col_chunk != b)
    def _():
        deliver(0).start()

    with jax.named_scope("drain_f"):
        bulk(15, fs, fr).wait_send()

    with jax.named_scope("swap"):

        @pl.when(col_chunk == b)
        def _():
            bulk(1, ds, dr).wait()

        @pl.when(col_chunk != b)
        def _():
            bulk(2, ds, dr).wait()

    value = (drecv[0] + drecv[1]) * scale
    row = lax.broadcasted_iota(jnp.int32, (64, 128), 0) + (g * 128 + c * 64)
    col = lax.broadcasted_iota(jnp.int32, (64, 128), 1) + b * 128
    out[...] = jnp.where(row == col, jnp.float32(0.0), value)


def body(coeffs):
    num_bands = coeffs.shape[3] // W * lax.axis_size("band")
    scale = W * K / num_bands
    dma = pltpu.SemaphoreType.DMA
    return pl.pallas_call(
        functools.partial(kernel, scale),
        name="coherence",
        out_shape=pltpu.VMEM((64, 128), F32),
        in_specs=[pl.BlockSpec(memory_space=pl.ANY)],
        out_specs=pl.BlockSpec(memory_space=pltpu.VMEM),
        scratch_shapes=[
            pltpu.VMEM((8, 2, 8, 64, 128), BF16),
            pltpu.VMEM((8, 8, 64, 256), BF16),
            pltpu.VMEM((8, 2, 8, 64, 256), BF16),
            pltpu.VMEM((8, 128, 256), BF16),
            pltpu.VMEM((8, 8, 128), F32),
            pltpu.VMEM((8, 8, 128), F32),
            pltpu.VMEM((8, 1024), F32),
            pltpu.VMEM((8, 64, 128), F32),
            pltpu.VMEM((8, 256, 1024), BF16),
            pltpu.VMEM((TILES, 64, 128), F32),
            pltpu.VMEM((TILES, 3, 64, 128), F32),
            pltpu.VMEM((TILES, 64, 128), F32),
            pltpu.VMEM((16, 64, 128), F32),
            pltpu.VMEM((128, 128), F32),
            pltpu.VMEM((128, 128), F32),
            pltpu.VMEM((64, 128), F32),
            pltpu.VMEM((2, 64, 128), F32),
            dma((3,)),
            dma,
            dma((8,)),
            dma,
            dma((8,)),
            dma,
            dma((8,)),
            dma((2,)),
            dma((8, 3)),
            dma,
            dma,
            dma,
            dma,
        ],
        compiler_params=pltpu.CompilerParams(
            collective_id=0, has_side_effects=True, vmem_limit_bytes=63 * 2**20
        ),
    )(coeffs)


def solution(mesh):
    return jax.shard_map(
        body,
        mesh=mesh,
        in_specs=(P(None, None, "chan", "band"),),
        out_specs=P("chan", "band"),
        check_vma=False,
    )
```
